768 devices in a mesh: rep: 12 (over z), own: 64 (over y, x, core).
Axes of the slice: x: 4, y: 8, z: 12, core: 2. Of those that a mesh axis runs over, the one named last changes fastest.
Arguments:
- grads: float32 [384, 576, 1024], P('rep', 'own'), may hold values from -60 to 60
- momentum: bfloat16 [768, 576, 1024], P(('rep', 'own')), may hold values from -6 to 6
- owner_table: int32 [12, 64], replicated, may hold values from 0 to 63, each once within a row
Outputs:
- new_momentum: bfloat16 [768, 576, 1024], P(('rep', 'own'))
- updates: bfloat16 [384, 576, 1024], P(None, 'own')
The draws below stay inside these ranges and needn't reach their ends.
Inputs may be any that keep to these rules, and one draw needn't show every extreme that they name: Each row of owner_table is a permutation of 0 to 63; entries of 32 or more mark empty slots.
All inputs are finite; a program needn't handle non-finite values.
Results may differ from the reference program's by a relative error of at most 0.01.
Values may be sent and summed in bfloat16 or wider, within the bound.
A program may use at most 128 MiB of HBM per device.

```python
import math
import jax
import jax.numpy as jnp
from jax import lax

MR = 576
MC = 1024
ITERS = 2
MATS = 32
MATS_ALL = 384
SLOTS = 768
N_REP = 12
N_OWN = 64


def draw_grads(key, part):
    keys = jax.random.split(jax.random.fold_in(key, 7), 3)
    base = jnp.clip(jax.random.normal(keys[0], (MATS_ALL, MR, MC), jnp.float32), -6.0, 6.0)
    row_scale = jnp.exp(jax.random.uniform(keys[1], (MATS_ALL, MR, 1), jnp.float32) * math.log(10.0))
    col_scale = jnp.exp(jax.random.uniform(keys[2], (MATS_ALL, 1, MC), jnp.float32) * math.log(10.0))
    return base * row_scale * col_scale * 0.1


def shard_levels(key, shape, pieces, smallest, top_value):
    gain, own = 1.0, jax.random.fold_in(key, 6)
    for axis_at, blocks in pieces:
        heights = jnp.exp(jax.random.uniform(jax.random.fold_in(own, axis_at), (blocks,), jnp.float32, smallest / len(pieces), top_value / len(pieces)))
        gain = gain * jnp.repeat(heights, shape[axis_at] // blocks).reshape([-1 if axis == axis_at else 1 for axis in range(len(shape))])
    return gain


def gaussian(key, extent, spread, bound, pieces=(), kind=jnp.bfloat16):
    loudness = shard_levels(key, extent, pieces, -0.22, 0.18) if pieces else 1.0
    values = jax.random.normal(key, extent, jnp.float32) * spread * loudness
    return jnp.minimum(jnp.maximum(values, -bound), bound).astype(kind)


def setup_inputs(seed: int = 0) -> dict:
    key_list = jax.random.split(jax.random.key(seed), 4)
    return {
        "grads": draw_grads(jax.random.fold_in(key_list[3], 71), 0),
        "momentum": gaussian(key_list[1], (SLOTS, MR, MC), 1.0, 6.0, ((0, 768),)),
        "owner_table": jax.vmap(lambda own: jax.random.permutation(own, N_OWN))(jax.random.split(key_list[2], N_REP)).reshape((N_REP, N_OWN)).astype(jnp.int32),
    }


DECAY = 0.95
COEF_A = 3.4445
COEF_B = -4.775
COEF_C = 2.0315
EPSILON = 1e-07

def orthogonalize(blend):
    total = jnp.sqrt(jnp.sum(blend * blend))
    iterate = (blend / (total + EPSILON)).astype(jnp.bfloat16)
    factor = 0.2 * math.sqrt(max(MR, MC))
    result = None
    for turn in range(ITERS):
        gram = jnp.dot(iterate, iterate.T, preferred_element_type=jnp.float32).astype(jnp.bfloat16)
        square = jnp.dot(gram, gram, preferred_element_type=jnp.float32)
        poly = (COEF_B * gram.astype(jnp.float32) + COEF_C * square).astype(jnp.bfloat16)
        mixed = COEF_A * iterate.astype(jnp.float32) + jnp.dot(poly, iterate, preferred_element_type=jnp.float32)
        if turn + 1 < ITERS:
            iterate = mixed.astype(jnp.bfloat16)
        else:
            result = (factor * mixed).astype(jnp.bfloat16)
    return result

def reference(grads, momentum, owner_table):
    half_grads = grads.astype(jnp.bfloat16)
    is_live = (owner_table < MATS).reshape(-1)
    clamped = jnp.minimum(owner_table, MATS - 1).astype(jnp.int32)
    source = (jnp.arange(N_REP, dtype=jnp.int32)[:, None] * MATS + clamped).reshape(-1).astype(jnp.int32)

    def slot_step(inputs):
        held, index, flag = inputs
        gradient = jnp.where(flag, half_grads[index].astype(jnp.float32), jnp.zeros((MR, MC), jnp.float32))
        return (DECAY * held.astype(jnp.float32) + gradient).astype(jnp.bfloat16)
    new_momentum = lax.map(slot_step, (momentum, source, is_live))
    inverse = jnp.argsort(owner_table, axis=1)[:, :MATS].astype(jnp.int32)
    slot_of = (jnp.arange(N_REP, dtype=jnp.int32)[:, None] * N_OWN + inverse).reshape(-1).astype(jnp.int32)

    def matrix_step(inputs):
        gradient_half, slot = inputs
        gradient = gradient_half.astype(jnp.float32)
        moment = DECAY * momentum[slot].astype(jnp.float32) + gradient
        return orthogonalize(gradient + DECAY * moment)
    updates = lax.map(matrix_step, (half_grads, slot_of))
    return (new_momentum, updates)
```

```python
import functools
import math

import jax
import jax.numpy as jnp
from jax import lax
from jax.experimental import pallas as pl
from jax.experimental.pallas import tpu as pltpu
from jax.sharding import PartitionSpec as P

ITERS = 2
DECAY = 0.95
COEF_A = 3.4445
COEF_B = -4.775
COEF_C = 2.0315
EPSILON = 1e-07
LANES = 128
MESH = pl.DeviceIdType.MESH

CHUNKS = (1, 2, 3, 3)
ORDER = (
    (0, 0), (0, 1), (1, 0), (0, 2), (1, 1), (0, 3), (1, 2), (0, 4),
    (2, 0), (1, 3), (0, 5), (2, 1), (1, 4), (3, 0), (2, 2), (1, 5),
    (3, 1), (2, 3), (3, 2), (2, 4), (3, 3), (2, 5), (3, 4), (3, 5),
)


def kernel(
    n_rep, n_own, mats,
    grads, momentum, table, new_momentum, updates,
    outgoing, incoming, blend, iterate, iterate2, gram, poly, rows_out,
    back0, back1, back2, back3, tile_a, tile_b, tile_c,
    send_in, recv_in, send_back, recv_back, send_ring, recv_ring,
):
    z, me = lax.axis_index("rep"), lax.axis_index("own")
    shard, _, cols = grads.shape
    rows = shard * n_own
    pieces = cols // LANES
    back = (back0, back1, back2, back3)
    up, down = lax.rem(z + 1, n_rep), lax.rem(z + n_rep - 1, n_rep)

    barrier = pltpu.get_barrier_semaphore()

    def greet(i, _):
        peer = lax.rem(me + i, n_own)
        pl.semaphore_signal(barrier, inc=1, device_id=(z, peer), device_id_type=MESH)
        return 0

    lax.fori_loop(1, n_own, greet, 0)
    for other in (up, down):
        pl.semaphore_signal(barrier, inc=1, device_id=(other, me), device_id_type=MESH)

    slots = jnp.broadcast_to(table[pl.ds(z, 1), :], (mats, n_own))
    matrices = lax.broadcasted_iota(jnp.int32, (mats, n_own), 0)
    holds = (slots == matrices).astype(jnp.float32)
    picks = holds.astype(jnp.bfloat16)
    spreads = holds.T.astype(jnp.bfloat16)

    def pack(j, _):
        for c in range(pieces):
            tile_a[pl.ds(c, n_own, stride=pieces), :] = jnp.dot(
                spreads,
                grads[j, :, c * LANES : (c + 1) * LANES].astype(jnp.bfloat16),
                preferred_element_type=jnp.float32,
            )
        outgoing[:, j] = tile_a[...].reshape(n_own, pieces, LANES).astype(jnp.bfloat16)
        return 0

    lax.fori_loop(0, shard, pack, 0)
    for j in range(shard):
        incoming[me * shard + j] = outgoing[me, j]
    pl.semaphore_wait(barrier, n_own + 1)

    def give(i, _):
        peer = lax.rem(me + i, n_own)
        pltpu.make_async_remote_copy(
            src_ref=outgoing.at[peer],
            dst_ref=incoming.at[pl.ds(me * shard, shard)],
            send_sem=send_in, recv_sem=recv_in, device_id=(z, peer), device_id_type=MESH,
        ).start()
        return 0

    lax.fori_loop(1, n_own, give, 0)
    pltpu.make_async_copy(
        incoming.at[pl.ds(0, (n_own - 1) * shard)], incoming.at[pl.ds(0, (n_own - 1) * shard)], recv_in
    ).wait()

    block = 16

    def combine(i, total):
        at = pl.multiple_of(i * block, block)
        tile_b[...] = incoming[pl.ds(at, block)].astype(jnp.float32).reshape(block * pieces, LANES)
        for c in range(pieces):
            here = (pl.ds(at, block), pl.ds(c * LANES, LANES))
            gradient = tile_b[pl.ds(c, block, stride=pieces), :]
            moment = DECAY * momentum[here].astype(jnp.float32) + gradient
            new_momentum[here] = moment.astype(jnp.bfloat16)
            mixed = gradient + DECAY * moment
            blend[here] = mixed
            total = total + mixed * mixed
        return total

    total = lax.fori_loop(0, rows // block, combine, jnp.zeros((block, LANES), jnp.float32))
    norm = jnp.sqrt(jnp.sum(total, keepdims=True))
    scale = 1.0 / (norm + EPSILON)

    def start(i, _):
        at = pl.ds(pl.multiple_of(i * block, block), block)
        iterate[at, :] = (blend[at, :] * scale).astype(jnp.bfloat16)
        return 0

    lax.fori_loop(0, rows // block, start, 0)

    band = rows // 3
    factor = 0.2 * math.sqrt(max(rows, cols))
    for turn in range(ITERS):
        now, later = (iterate, iterate2) if turn % 2 == 0 else (iterate2, iterate)

        def gram_band(i, _):
            at = pl.ds(pl.multiple_of(i * band, band), band)
            gram[at, :] = lax.dot_general(
                now[at, :], now[...], (((1,), (1,)), ((), ())), preferred_element_type=jnp.float32
            ).astype(jnp.bfloat16)
            return 0

        lax.fori_loop(0, 3, gram_band, 0)

        def poly_band(i, _):
            at = pl.ds(pl.multiple_of(i * band, band), band)
            mine = gram[at, :]
            square = jnp.dot(mine, gram[...], preferred_element_type=jnp.float32)
            poly[at, :] = (COEF_B * mine.astype(jnp.float32) + COEF_C * square).astype(jnp.bfloat16)
            return 0

        lax.fori_loop(0, 3, poly_band, 0)

        def mixed_band(i, _):
            at = pl.ds(pl.multiple_of(i * band, band), band)
            for wide in range(0, cols, 256):
                mixed = COEF_A * now[at, wide : wide + 256].astype(jnp.float32) + jnp.dot(
                    poly[at, :], now[:, wide : wide + 256], preferred_element_type=jnp.float32
                )
                if turn + 1 < ITERS:
                    later[at, wide : wide + 256] = mixed.astype(jnp.bfloat16)
                else:
                    mixed = factor * mixed
                    for c in range(2):
                        tile_c[pl.ds(wide // LANES + c, band, stride=pieces), :] = mixed[
                            :, c * LANES : (c + 1) * LANES
                        ]
            if turn + 1 == ITERS:

                def to_tiles(t, _):
                    piece = tile_c[pl.ds(pl.multiple_of(t * 8 * pieces, 8 * pieces), 8 * pieces), :]
                    rows_out[pl.ds(i * band + t * 8, 8)] = piece.reshape(8, pieces, LANES).astype(jnp.bfloat16)
                    return 0

                lax.fori_loop(0, band // 8, to_tiles, 0)
            return 0

        lax.fori_loop(0, 3, mixed_band, 0)

    first = 0
    firsts = []
    for q, count in enumerate(CHUNKS):
        firsts.append(first)
        back[q][me] = rows_out[pl.ds(me * shard + first, count)]

        def give_back(i, _):
            peer = lax.rem(me + i, n_own)
            pltpu.make_async_remote_copy(
                src_ref=rows_out.at[pl.ds(peer * shard + first, count)],
                dst_ref=back[q].at[me],
                send_sem=send_back.at[q], recv_sem=recv_back.at[q],
                device_id=(z, peer), device_id_type=MESH,
            ).start()
            return 0

        lax.fori_loop(1, n_own, give_back, 0)
        first += count

    half = mats // 2
    last = n_rep // 2 - 1

    def ring(q, step, way):
        source = lax.rem(z + n_rep - step, n_rep) if way == 0 else lax.rem(z + step, n_rep)
        at, count = source * mats, mats
        if step == last:
            at, count = at + way * half, half
        where = updates.at[
            pl.ds(firsts[q], CHUNKS[q]), pl.ds(pl.multiple_of(at, half), count), :
        ]
        return pltpu.make_async_remote_copy(
            src_ref=where, dst_ref=where,
            send_sem=send_ring.at[q, step, way], recv_sem=recv_ring.at[q, step, way],
            device_id=(up if way == 0 else down, me), device_id_type=MESH,
        )

    def arrival(q, step, way):
        source = lax.rem(z + 2 * n_rep - step - 1, n_rep) if way == 0 else lax.rem(z + step + 1, n_rep)
        at, count = source * mats, mats
        if step == last:
            at, count = at + way * half, half
        where = updates.at[
            pl.ds(firsts[q], CHUNKS[q]), pl.ds(pl.multiple_of(at, half), count), :
        ]
        return pltpu.make_async_copy(where, where, recv_ring.at[q, step, way])

    for q, step in ORDER:
        if step == 0:
            got = back[q].at[pl.ds(0, n_own - 1)]
            pltpu.make_async_copy(got, got, recv_back.at[q]).wait()
            for j in range(CHUNKS[q]):

                tile_a[...] = back[q][:, j].astype(jnp.float32).reshape(n_own * pieces, LANES)
                for c in range(pieces):
                    updates[
                        firsts[q] + j, pl.ds(pl.multiple_of(z * mats, mats), mats), c * LANES : (c + 1) * LANES
                    ] = jnp.dot(
                        picks,
                        tile_a[pl.ds(c, n_own, stride=pieces), :].astype(jnp.bfloat16),
                        preferred_element_type=jnp.float32,
                    ).astype(jnp.bfloat16)
        for way in range(2):
            if step > 0:
                arrival(q, step - 1, way).wait()
            ring(q, step, way).start()
    for q in range(len(CHUNKS)):
        for way in range(2):
            arrival(q, last, way).wait()

    pltpu.make_async_copy(
        outgoing.at[pl.ds(0, n_own - 1)], outgoing.at[pl.ds(0, n_own - 1)], send_in
    ).wait()
    for q in range(len(CHUNKS)):
        sent = back[q].at[pl.ds(0, n_own - 1)]
        pltpu.make_async_copy(sent, sent, send_back.at[q]).wait()
        for step in range(last + 1):
            for way in range(2):
                ring(q, step, way).wait_send()


def body(grads, momentum, owner_table):
    n_rep, n_own = lax.axis_size("rep"), lax.axis_size("own")
    mats, shard, cols = grads.shape
    rows = shard * n_own
    pieces = cols // LANES
    vmem = pl.BlockSpec(memory_space=pltpu.VMEM)
    tile = (pieces, LANES)
    chunks = len(CHUNKS)
    new_momentum, updates = pl.pallas_call(
        functools.partial(kernel, n_rep, n_own, mats),
        out_shape=(
            jax.ShapeDtypeStruct((rows, cols), jnp.bfloat16),
            jax.ShapeDtypeStruct((shard, n_rep * mats, cols), jnp.bfloat16),
        ),
        in_specs=[vmem, vmem, vmem],
        out_specs=(vmem, vmem),
        scratch_shapes=[
            pltpu.VMEM((n_own, shard, *tile), jnp.bfloat16),
            pltpu.VMEM((rows, *tile), jnp.bfloat16),
            pltpu.VMEM((rows, cols), jnp.float32),
            pltpu.VMEM((rows, cols), jnp.bfloat16),
            pltpu.VMEM((rows, cols), jnp.bfloat16),
            pltpu.VMEM((rows, rows), jnp.bfloat16),
            pltpu.VMEM((rows, rows), jnp.bfloat16),
            pltpu.VMEM((rows, *tile), jnp.bfloat16),
            *(pltpu.VMEM((n_own, count, *tile), jnp.bfloat16) for count in CHUNKS),
            pltpu.VMEM((n_own * pieces, LANES), jnp.float32),
            pltpu.VMEM((16 * pieces, LANES), jnp.float32),
            pltpu.VMEM((rows // 3 * pieces, LANES), jnp.float32),
            pltpu.SemaphoreType.DMA,
            pltpu.SemaphoreType.DMA,
            pltpu.SemaphoreType.DMA((chunks,)),
            pltpu.SemaphoreType.DMA((chunks,)),
            pltpu.SemaphoreType.DMA((chunks, n_rep // 2, 2)),
            pltpu.SemaphoreType.DMA((chunks, n_rep // 2, 2)),
        ],
        compiler_params=pltpu.CompilerParams(
            collective_id=0, has_side_effects=True, vmem_limit_bytes=40 * 1024 * 1024
        ),
    )(jnp.transpose(grads, (1, 0, 2)), momentum[0], owner_table)
    return (new_momentum[None], jnp.transpose(updates, (1, 0, 2)))


def solution(mesh):
    return jax.shard_map(
        body,
        mesh=mesh,
        in_specs=(P("rep", "own", None), P(("rep", "own"), None, None), P()),
        out_specs=(P(("rep", "own"), None, None), P(None, "own", None)),
        check_vma=False,
    )
```
